32 devices in a mesh: patch: 16 (over z, y, x), shell: 2 (over core).
Axes of the slice: x: 2, y: 2, z: 4, core: 2. Of those that a mesh axis runs over, the one named last changes fastest.
Arguments:
- velocity: float32 [3, 64, 16, 512], P(None, 'patch', None, 'shell'), may hold values from -4 to 4
- pressure: float32 [4, 32, 8, 256], P(None, 'patch', None, 'shell'), may hold values from -6 to 6
- force: float32 [3, 64, 16, 512], P(None, 'patch', None, 'shell'), may hold values from -6 to 6
- viscosity: float32 [32, 8, 256], P('patch', None, 'shell'), may hold values from 0.1 to 10
- element_stiffness: float32 [81, 81], replicated, as said below
- element_divergence: float32 [4, 81], replicated, may hold values from -0.625 to 0.625
Outputs:
- solution: float32 [3, 64, 16, 512], P(None, 'patch', None, 'shell')
- new_pressure: float32 [4, 32, 8, 256], P(None, 'patch', None, 'shell')
The draws below stay inside these ranges and needn't reach their ends.
Inputs may be any that keep to these rules, and one draw needn't show every extreme that they name: `element_stiffness`: symmetric and positive definite.
All inputs are finite; a program needn't handle non-finite values.
Results may differ from the reference program's by a relative error of at most 0.0003.
Values sent between devices are 32-bit elements; how exact they have to be, the bound alone decides.
A program may use at most 64 MiB of HBM per device.

```python
import math
import jax
import jax.numpy as jnp
from jax import lax

EA = 2
EB = 8
ER = 128
ITERS = 2
LA = 32
LR = 256
NA = 64
NB = 16
NR = 512
N_PATCH = 16
N_SHELL = 2


def draw_element_stiffness(key, part):
    factor = jax.random.normal(key, (81, 81), jnp.float32)
    gram = jnp.dot(factor, factor.T, precision=lax.Precision.HIGHEST) / 81.0
    return gram + 0.5 * jnp.eye(81, dtype=jnp.float32)


def shard_levels(stream_key, shape, shards, low, top_value):
    loudness = 1.0
    for axis_at, parts in shards:
        draws = jax.random.uniform(jax.random.fold_in(jax.random.fold_in(stream_key, 6), axis_at), (parts,), jnp.float32, low / len(shards), top_value / len(shards))
        loudness = loudness * jnp.repeat(jnp.exp(draws), shape[axis_at] // parts).reshape((-1,) + (1,) * (len(shape) - 1 - axis_at))
    return loudness


def bell_draw(stream_key, dims, width, most, cuts=(), kind=jnp.bfloat16):
    result = width * jax.random.normal(stream_key, dims, jnp.float32)
    if cuts:
        result = result * shard_levels(stream_key, dims, cuts, -0.22, 0.18)
    return jnp.clip(result, -most, most).astype(kind)


def setup_inputs(seed: int = 0) -> dict:
    streams_of = jax.random.split(jax.random.key(seed), 7)
    velocity = bell_draw(streams_of[0], (3, NA, NB, NR), 0.5, 4.0, ((1, 16), (3, 2)), jnp.float32)
    pressure = bell_draw(streams_of[1], (4, LA, EB, LR), 1.0, 6.0, ((1, 16), (3, 2)), jnp.float32)
    force = bell_draw(streams_of[2], (3, NA, NB, NR), 1.0, 6.0, ((1, 16), (3, 2)), jnp.float32)
    viscosity = jnp.clip(jnp.exp(math.log(10.0) - 4.6051702 * jax.random.uniform(streams_of[3], (LA, EB, LR), jnp.float32) ** shard_levels(streams_of[3], (LA, EB, LR), ((0, 16), (2, 2)), -0.2, 0.2)), 0.1, 10.0)
    element_stiffness = draw_element_stiffness(jax.random.fold_in(streams_of[6], 71), 0)
    element_divergence = bell_draw(streams_of[5], (4, 81), 81 ** -0.5, 0.625, (), jnp.float32)
    return {"velocity": velocity, "pressure": pressure, "force": force, "viscosity": viscosity, "element_stiffness": element_stiffness, "element_divergence": element_divergence}


relaxation = 1.0


def alternate(part_low, part_mid, part_high, along_axis):
    half_len = part_low.shape[along_axis]
    plane_shape = list(part_low.shape)
    plane_shape[along_axis] = 1
    zero_plane = jnp.zeros(plane_shape, part_low.dtype)
    even_sum = jnp.concatenate([part_low, zero_plane], along_axis) + jnp.concatenate([zero_plane, part_high], along_axis)
    even_head = lax.slice_in_dim(even_sum, 0, half_len, 1, along_axis)
    paired = jnp.stack([even_head, part_mid], axis=along_axis + 1)
    new_shape = list(part_low.shape)
    new_shape[along_axis] = 2 * half_len
    merged = paired.reshape(new_shape)
    return jnp.concatenate([merged, lax.slice_in_dim(even_sum, half_len, half_len + 1, 1, along_axis)], along_axis)


def element_values(extended, elem_a, elem_b, elem_r):
    gathered = []
    for offset_a in range(3):
        slab_a = lax.slice_in_dim(extended, offset_a, offset_a + 2 * elem_a - 1, 2, 1)
        for offset_b in range(3):
            slab_b = lax.slice_in_dim(slab_a, offset_b, offset_b + 2 * elem_b - 1, 2, 2)
            for offset_r in range(3):
                gathered.append(lax.slice_in_dim(slab_b, offset_r, offset_r + 2 * elem_r - 1, 2, 3))
    return jnp.stack(gathered, axis=1).reshape(81, elem_a * elem_b * elem_r)


def assemble(element_terms, elem_a, elem_b, elem_r):
    split_terms = element_terms.reshape(3, 3, 3, 3, elem_a, elem_b, elem_r)
    radial_sum = alternate(split_terms[:, :, :, 0], split_terms[:, :, :, 1], split_terms[:, :, :, 2], 5)
    middle_sum = alternate(radial_sum[:, :, 0], radial_sum[:, :, 1], radial_sum[:, :, 2], 3)
    return alternate(middle_sum[:, 0], middle_sum[:, 1], middle_sum[:, 2], 1)


def element_terms_of(values, stiffness, divergence_map, visc_flat, pressure_flat):
    element_terms = jnp.dot(stiffness, values, precision=lax.Precision.HIGHEST, preferred_element_type=jnp.float32) * visc_flat[None, :]
    if pressure_flat is not None:
        element_terms = element_terms + jnp.dot(divergence_map.T, pressure_flat, precision=lax.Precision.HIGHEST, preferred_element_type=jnp.float32)
    return element_terms


def extend_global(nodal_field):
    wrapped = jnp.concatenate([nodal_field, nodal_field[:, :1]], axis=1)
    zero_b = jnp.zeros((3, wrapped.shape[1], 1, wrapped.shape[3]), jnp.float32)
    wrapped = jnp.concatenate([wrapped, zero_b], axis=2)
    zero_r = jnp.zeros((3, wrapped.shape[1], wrapped.shape[2], 1), jnp.float32)
    return jnp.concatenate([wrapped, zero_r], axis=3)


def patch_apply(extended, viscosity, pressure, stiffness, divergence_map, with_pressure):
    radial_elems = ER * N_SHELL

    def one_patch(index):
        block_ext = lax.dynamic_slice_in_dim(extended, (index * (2 * EA)).astype(jnp.int32), 2 * EA + 1, 1)
        visc_block = lax.dynamic_slice_in_dim(viscosity, (index * EA).astype(jnp.int32), EA, 0).reshape(EA * EB * radial_elems)
        values = element_values(block_ext, EA, EB, radial_elems)
        pres_block = None
        if with_pressure:
            pres_block = lax.dynamic_slice_in_dim(pressure, (index * EA).astype(jnp.int32), EA, 1).reshape(4, EA * EB * radial_elems)
        return assemble(element_terms_of(values, stiffness, divergence_map, visc_block, pres_block), EA, EB, radial_elems)

    stacked = lax.map(one_patch, jnp.arange(N_PATCH, dtype=jnp.int32))
    main_part = stacked[:, :, :2 * EA, :2 * EB, :2 * radial_elems]
    extra_plane = stacked[:, :, 2 * EA, :2 * EB, :2 * radial_elems]
    rolled = jnp.roll(extra_plane, 1, axis=0)
    main_part = jnp.concatenate([main_part[:, :, :1] + rolled[:, :, None], main_part[:, :, 1:]], axis=2)
    return jnp.transpose(main_part, (1, 0, 2, 3, 4)).reshape(3, N_PATCH * 2 * EA, 2 * EB, 2 * radial_elems)


def global_divergence(extended, divergence_map):
    radial_elems = ER * N_SHELL

    def one_patch(index):
        block_ext = lax.dynamic_slice_in_dim(extended, (index * (2 * EA)).astype(jnp.int32), 2 * EA + 1, 1)
        values = element_values(block_ext, EA, EB, radial_elems)
        return jnp.dot(divergence_map, values, precision=lax.Precision.HIGHEST, preferred_element_type=jnp.float32)

    stacked = lax.map(one_patch, jnp.arange(N_PATCH, dtype=jnp.int32))
    stacked = stacked.reshape(N_PATCH, 4, EA, EB, radial_elems)
    return jnp.transpose(stacked, (1, 0, 2, 3, 4)).reshape(4, N_PATCH * EA, EB, radial_elems)


def reference(velocity, pressure, force, viscosity, element_stiffness, element_divergence):
    solution = velocity
    new_pressure = pressure
    extended = extend_global(solution)
    for iteration in range(ITERS):
        image_u = patch_apply(extended, viscosity, new_pressure, element_stiffness, element_divergence, True)
        residual = force - image_u
        residual_ext = extend_global(residual)
        image_r = patch_apply(residual_ext, viscosity, None, element_stiffness, element_divergence, False)
        step_size = jnp.sum(residual * residual) / jnp.sum(residual * image_r)
        solution = solution + step_size * residual
        extended = extend_global(solution)
        divergence = global_divergence(extended, element_divergence)
        new_pressure = new_pressure + relaxation * divergence / viscosity[None]
    return solution, new_pressure
```

```python
import functools

import jax
import jax.numpy as jnp
import numpy as np
from jax import lax
from jax.experimental import pallas as pl
from jax.experimental.pallas import tpu as pltpu
from jax.sharding import PartitionSpec as P

ITERS = 2
MESH = pl.DeviceIdType.MESH
SLOTS = 16
F32 = jnp.float32
BF16 = jnp.bfloat16


def unknown_map():
    rows = np.zeros((9 * SLOTS, 81), np.float32)
    for x in range(3):
        for a in range(3):
            for b in range(3):
                for c in range(3):
                    rows[(b * 3 + a) * SLOTS + c * 3 + x, x * 27 + a * 9 + b * 3 + c] = 1.0
    return rows


def dot(x, y, contract=((1,), (0,))):
    return lax.dot_general(x, y, (contract, ((), ())), preferred_element_type=F32)


def split2(x):
    hi = x.astype(BF16)
    return hi, (x - hi.astype(F32)).astype(BF16)


def exact_dot(x, perm):
    hi, mid = split2(x)
    lo = (x - hi.astype(F32) - mid.astype(F32)).astype(BF16)
    return dot(hi, perm) + dot(mid, perm) + dot(lo, perm)


def kernel(
    dims,
    v_ref, p_ref, f_ref, visc_ref, stiff_ref, div_ref, map_ref,
    sol_ref, pout_ref,
    fld, fhi, flo, out, out2, pq, bvals,
    vplane, vcol, vcol_in, vdiag_in,
    col_out, col_in, plane_out, plane_in, gcol_out, gcol_in, sums,
    bar_send, bar_recv, col_send, col_recv, pl_send, pl_recv, ar_send, ar_recv,
):
    n_patch, n_shell, ea, eb, na, nb, lanes = dims
    n_dev = n_patch * n_shell
    planes = na + 1
    block = 3 * nb
    owned = na * block
    rows = planes * block
    width = vcol.shape[1]
    stride = planes * SLOTS
    patch = lax.axis_index("patch")
    shell = lax.axis_index("shell")
    after = lax.rem(patch + 1, n_patch)
    before = lax.rem(patch + n_patch - 1, n_patch)
    has_above = shell < n_shell - 1
    has_below = shell > 0
    above = jnp.minimum(shell + 1, n_shell - 1)
    below = jnp.maximum(shell - 1, 0)

    def remote(src, dst, send, recv, to_patch, to_shell):
        return pltpu.make_async_remote_copy(
            src_ref=src, dst_ref=dst, send_sem=send, recv_sem=recv,
            device_id={"patch": to_patch, "shell": to_shell}, device_id_type=MESH,
        )

    plane_copy = remote(v_ref.at[:, 0], vplane, bar_send.at[0], bar_recv.at[0], before, shell)
    plane_copy.start()
    head = jnp.concatenate(
        [v_ref[x, a, :, :lanes] for a in range(na) for x in range(3)]
        + [jnp.zeros((width - owned, lanes), F32)], axis=0)
    vcol[...] = jnp.transpose(head)[:8]
    col_copy = remote(vcol, vcol_in, bar_send.at[1], bar_recv.at[1], patch, below)
    diag_copy = remote(vcol, vdiag_in, bar_send.at[2], bar_recv.at[2], before, below)

    @pl.when(has_below)
    def _():
        col_copy.start()
        diag_copy.start()

    row_map = map_ref[...].astype(BF16)
    a_hi, a_lo = split2(stiff_ref[...])
    div = jnp.concatenate([div_ref[...], jnp.zeros((4, 81), F32)], axis=0)
    b_hi = div.astype(BF16).astype(F32)
    b_lo = (div - b_hi).astype(BF16).astype(F32)

    def both_sides(mat):
        return dot(dot(row_map, mat).astype(BF16), row_map, ((1,), (1,)))

    def right_side(mat):
        return dot(mat.astype(BF16), row_map, ((1,), (1,)))

    apply_hi = jnp.concatenate([both_sides(a_hi), right_side(b_hi)], axis=0).astype(BF16)
    apply_lo = jnp.concatenate([both_sides(a_lo), right_side(b_lo)], axis=0).astype(BF16)
    apply_all = jnp.concatenate([apply_hi, apply_lo], axis=0)
    b_stack = jnp.concatenate([b_hi, b_lo, b_hi, jnp.zeros((8, 81), F32)], axis=0).astype(BF16)
    back = dot(row_map, b_stack, ((1,), (1,))).astype(BF16)
    m_rows = 9 * SLOTS
    span = 3 * SLOTS

    r_i = lax.broadcasted_iota(jnp.int32, (2 * lanes, 2 * lanes), 0)
    c_i = lax.broadcasted_iota(jnp.int32, (2 * lanes, 2 * lanes), 1)
    unzip = (r_i == jnp.where(c_i < lanes, 2 * c_i, 2 * c_i - 2 * lanes + 1)).astype(BF16)
    rezip = (c_i == jnp.where(r_i < lanes, 2 * r_i, 2 * r_i - 2 * lanes + 1)).astype(BF16)

    fld[...] = jnp.zeros_like(fld)
    pq[...] = jnp.zeros_like(pq)
    for i in range(ea):
        for q in range(4):
            pq[pl.ds(i * eb * 8 + q, eb, stride=8), :] = p_ref[q, i]
    inv_visc = [1.0 / visc_ref[i] for i in range(ea)]
    visc = [visc_ref[i] for i in range(ea)]

    f_n = exact_dot(jnp.concatenate(
        [f_ref[x, a] for a in range(na) for x in range(3)], axis=0), unzip)
    zero_plane = jnp.zeros((block, lanes), F32)
    f_e = jnp.concatenate([f_n[:, :lanes], zero_plane], axis=0)
    f_o = jnp.concatenate([f_n[:, lanes:], zero_plane], axis=0)
    v_own = exact_dot(jnp.concatenate(
        [v_ref[x, a] for a in range(na) for x in range(3)], axis=0), unzip)

    lane_n = lax.broadcasted_iota(jnp.int32, (rows, lanes), 1)
    col_lane = lax.broadcasted_iota(jnp.int32, (1, width), 1)

    def column(row):
        return jnp.transpose(jnp.broadcast_to(row, (lanes, width)))[:rows]

    def put(even, odd, ghost):
        shifted = pltpu.roll(jnp.where(lane_n == 0, column(ghost), even), lanes - 1, 1)
        for a in range(planes):
            for x in range(3):
                at = (a * 3 + x) * nb
                for c, part in ((0, even), (1, odd), (2, shifted)):
                    fld[pl.ds(a * SLOTS + c * 3 + x, nb, stride=stride), :] = part[at:at + nb]
        hi, lo = split2(fld[...])
        fhi[...] = hi
        flo[...] = lo

    def gathered(ref, j):
        parts = []
        for i in range(ea):
            parts.append(jnp.concatenate(
                [ref[(2 * j + b) * stride + 2 * i * SLOTS:(2 * j + b) * stride + 2 * i * SLOTS + span]
                 for b in range(3)], axis=0))
        return jnp.concatenate(parts, axis=1)

    def back_apply(pieces):
        packed = []
        for w in pieces:
            hi = w.astype(BF16).astype(F32)
            packed.append(jnp.concatenate([hi, hi, w - hi, jnp.zeros_like(w)], axis=0))
        return dot(back, jnp.concatenate(packed, axis=1).astype(BF16))

    def add_to(ref, terms, i, j):
        for b in range(3):
            at = (2 * j + b) * stride + 2 * i * SLOTS
            ref[at:at + span] = ref[at:at + span] + terms[b * span:(b + 1) * span]

    def operator(mode, slot):
        if mode != "last":
            out[...] = jnp.zeros_like(out)
        if mode == "first":
            out2[...] = jnp.zeros_like(out2)
        energy = jnp.zeros((8, lanes), F32)
        for j in range(eb):
            hi = dot(apply_all, gathered(fhi, j))
            full = hi[:m_rows + 8] + hi[m_rows + 8:] + dot(apply_hi, gathered(flo, j))
            scaled = []
            for i in range(ea):
                part = full[:, i * lanes:(i + 1) * lanes]
                at = (i * eb + j) * 8
                bv = part[m_rows:]
                bvals[slot, at:at + 8] = bv
                scaled.append(bv * inv_visc[i][j:j + 1])
            if mode == "first":
                pres = [pq[(i * eb + j) * 8:(i * eb + j) * 8 + 8] for i in range(ea)]
                extra = back_apply(pres + scaled)
            elif mode == "second":
                extra = back_apply(scaled)
            for i in range(ea):
                terms = full[:m_rows, i * lanes:(i + 1) * lanes] * visc[i][j:j + 1]
                if mode != "first":
                    vals = jnp.concatenate(
                        [fld[(2 * j + b) * stride + 2 * i * SLOTS:
                             (2 * j + b) * stride + 2 * i * SLOTS + span] for b in range(3)], axis=0)
                    energy = energy + jnp.sum((terms * vals).reshape(m_rows // 8, 8, lanes), axis=0)
                if mode != "last":
                    add_to(out, terms + extra[:, i * lanes:(i + 1) * lanes], i, j)
                if mode == "first":
                    add_to(out2, extra[:, (ea + i) * lanes:(ea + i + 1) * lanes], i, j)
        return energy

    def collect(ref, c):
        return jnp.concatenate(
            [ref[pl.ds(a * SLOTS + c * 3 + x, nb, stride=stride), :]
             for a in range(planes) for x in range(3)], axis=0)

    def padded(part):
        return jnp.concatenate([part, jnp.zeros((width - rows, lanes), F32)], axis=0)

    def complete(fields, base):
        count = len(fields)
        span_f = slice(base, base + count)
        own_low, own_high = [], []
        for n, (even, odd, carry) in enumerate(fields):
            low = jnp.transpose(padded(even))[:8]
            high = jnp.transpose(padded(carry))[lanes - 8:]
            col_out[0, base + n] = low
            col_out[1, base + n] = high
            own_high.append(high[7:8])
        phase = 0 if base == 0 else 1
        down = remote(col_out.at[0, span_f], col_in.at[0, span_f],
                      col_send.at[phase, 0], col_recv.at[phase, 0], patch, below)
        up = remote(col_out.at[1, span_f], col_in.at[1, span_f],
                    col_send.at[phase, 1], col_recv.at[phase, 1], patch, above)

        @pl.when(has_below)
        def _():
            down.start()

        @pl.when(has_above)
        def _():
            up.start()

        @pl.when(has_above)
        def _():
            down.wait_recv()

        @pl.when(jnp.logical_not(has_above))
        def _():
            col_in[0, span_f] = jnp.zeros((count, 8, width), F32)

        @pl.when(has_below)
        def _():
            up.wait_recv()

        @pl.when(jnp.logical_not(has_below))
        def _():
            col_in[1, span_f] = jnp.zeros((count, 8, width), F32)

        halves = []
        for n, (even, odd, carry) in enumerate(fields):
            from_below = column(col_in[1, base + n][7:8])
            even = even + pltpu.roll(jnp.where(lane_n == lanes - 1, from_below, carry), 1, 1)
            ghost = jnp.where(has_above, own_high[n] + col_in[0, base + n][0:1], 0.0)
            halves.append((even, odd, ghost))
            for side, at in ((0, 0), (1, owned)):
                plane_out[side, base + n, 0] = even[at:at + block]
                plane_out[side, base + n, 1] = odd[at:at + block]
            gcol_out[base + n] = jnp.broadcast_to(ghost, (8, width))
        copies = []
        for side, to in ((0, before), (1, after)):
            copies.append(remote(plane_out.at[side, span_f], plane_in.at[side, span_f],
                                 pl_send.at[phase, side, 0], pl_recv.at[phase, side, 0], to, shell))
            copies.append(remote(gcol_out.at[span_f], gcol_in.at[side, span_f],
                                 pl_send.at[phase, side, 1], pl_recv.at[phase, side, 1], to, shell))
        for copy in copies:
            copy.start()

        @pl.when(has_below)
        def _():
            down.wait_send()

        @pl.when(has_above)
        def _():
            up.wait_send()

        for copy in copies:
            copy.wait()
        done = []
        for n, (even, odd, ghost) in enumerate(halves):
            def joined(part, k):
                return jnp.concatenate(
                    [part[:block] + plane_in[1, base + n, k], part[block:owned],
                     part[owned:] + plane_in[0, base + n, k]], axis=0)
            first = pltpu.roll(gcol_in[1, base + n], width - owned, 1)[0:1]
            last = pltpu.roll(gcol_in[0, base + n], owned, 1)[0:1]
            ghost = ghost + jnp.where(col_lane < block, first, 0.0)
            ghost = ghost + jnp.where(
                jnp.logical_and(col_lane >= owned, col_lane < rows), last, 0.0)
            done.append((joined(even, 0), joined(odd, 1), ghost))
        return done

    me = patch * n_shell + shell

    def norm_of(even, odd):
        sq = even[:owned] * even[:owned] + odd[:owned] * odd[:owned]
        return jnp.sum(sq.reshape(owned // 8, 8, lanes), axis=0)

    def sums_start(phase, norm, energy):
        sums[phase, me] = jnp.concatenate(
            [jnp.sum(norm, axis=0, keepdims=True), jnp.sum(energy, axis=0, keepdims=True)], axis=0)

        @pl.loop(1, n_dev)
        def _(d):
            to = lax.rem(me + d, n_dev)
            remote(sums.at[phase, me], sums.at[phase, me], ar_send.at[phase], ar_recv.at[phase],
                   lax.div(to, n_shell), lax.rem(to, n_shell)).start()

    def sums_end(phase):
        whole = sums.at[phase, pl.ds(0, n_dev - 1)]
        pltpu.make_async_copy(whole, whole, ar_send.at[phase]).wait()
        pltpu.make_async_copy(whole, whole, ar_recv.at[phase]).wait()
        total = jnp.sum(sums[phase], axis=0)
        total = jnp.sum(total, axis=1, keepdims=True)
        return total[0:1] / total[1:2]

    plane_copy.wait()

    @pl.when(has_below)
    def _():
        col_copy.wait_send()
        diag_copy.wait_send()

    @pl.when(has_above)
    def _():
        col_copy.wait_recv()
        diag_copy.wait_recv()

    @pl.when(jnp.logical_not(has_above))
    def _():
        vcol_in[...] = jnp.zeros_like(vcol_in)
        vdiag_in[...] = jnp.zeros_like(vdiag_in)

    v_next = exact_dot(jnp.concatenate([vplane[x] for x in range(3)], axis=0), unzip)
    v_e = jnp.concatenate([v_own[:, :lanes], v_next[:, :lanes]], axis=0)
    v_o = jnp.concatenate([v_own[:, lanes:], v_next[:, lanes:]], axis=0)
    v_g = jnp.where(col_lane < owned, vcol_in[0:1], pltpu.roll(vdiag_in[...], owned, 1)[0:1])
    put(v_e, v_o, v_g)

    operator("first", 0)
    first = (f_e - collect(out, 0), f_o - collect(out, 1), -collect(out, 2))
    second = tuple(x - collect(out2, c) for c, x in enumerate(first))
    r0, s0 = complete([first, second], 0)
    put(*r0)
    energy = operator("second", 1)
    sums_start(0, norm_of(r0[0], r0[1]), energy)
    (h0,) = complete([tuple(collect(out, c) for c in range(3))], 2)
    step0 = sums_end(0)
    r1 = tuple(s - step0 * h for s, h in zip(s0, h0))
    put(*r1)
    energy = operator("last", 2)
    sums_start(1, norm_of(r1[0], r1[1]), energy)
    part_e = (v_e + step0 * r0[0])[:owned]
    part_o = (v_o + step0 * r0[1])[:owned]
    step1 = sums_end(1)
    result = exact_dot(jnp.concatenate(
        [part_e + step1 * r1[0][:owned], part_o + step1 * r1[1][:owned]], axis=1), rezip)
    for a in range(na):
        for x in range(3):
            at = (a * 3 + x) * nb
            sol_ref[x, a] = result[at:at + nb]
    bvals[0] = 2.0 * (bvals[0] + step0 * bvals[1]) + step1 * bvals[2]
    for i in range(ea):
        for q in range(4):
            pout_ref[q, i] = p_ref[q, i] + bvals[0, pl.ds(i * eb * 8 + q, eb, stride=8), :] * inv_visc[i]


def solution(mesh):
    n_patch, n_shell = mesh.shape["patch"], mesh.shape["shell"]
    row_map = unknown_map()

    def per_device(velocity, pressure, force, viscosity, element_stiffness, element_divergence):
        ea, eb, lanes = viscosity.shape
        na, nb = velocity.shape[1], velocity.shape[2]
        dims = (n_patch, n_shell, ea, eb, na, nb, lanes)
        block = 3 * nb
        width = -(-(na + 1) * block // 128) * 128
        g_rows = (nb + 1) * (na + 1) * SLOTS
        vmem = pl.BlockSpec(memory_space=pltpu.VMEM)
        return pl.pallas_call(
            functools.partial(kernel, dims),
            out_shape=(jax.ShapeDtypeStruct(velocity.shape, F32),
                       jax.ShapeDtypeStruct(pressure.shape, F32)),
            in_specs=[vmem] * 7,
            out_specs=(vmem, vmem),
            scratch_shapes=[
                pltpu.VMEM((g_rows, lanes), F32),
                pltpu.VMEM((g_rows, lanes), BF16),
                pltpu.VMEM((g_rows, lanes), BF16),
                pltpu.VMEM((g_rows, lanes), F32),
                pltpu.VMEM((g_rows, lanes), F32),
                pltpu.VMEM((ea * eb * 8, lanes), F32),
                pltpu.VMEM((3, ea * eb * 8, lanes), F32),
                pltpu.VMEM((3, nb, 2 * lanes), F32),
                pltpu.VMEM((8, width), F32),
                pltpu.VMEM((8, width), F32),
                pltpu.VMEM((8, width), F32),
                pltpu.VMEM((2, 3, 8, width), F32),
                pltpu.VMEM((2, 3, 8, width), F32),
                pltpu.VMEM((2, 3, 2, block, lanes), F32),
                pltpu.VMEM((2, 3, 2, block, lanes), F32),
                pltpu.VMEM((3, 8, width), F32),
                pltpu.VMEM((2, 3, 8, width), F32),
                pltpu.VMEM((2, n_patch * n_shell, 2, lanes), F32),
                pltpu.SemaphoreType.DMA((3,)),
                pltpu.SemaphoreType.DMA((3,)),
                pltpu.SemaphoreType.DMA((2, 2)),
                pltpu.SemaphoreType.DMA((2, 2)),
                pltpu.SemaphoreType.DMA((2, 2, 2)),
                pltpu.SemaphoreType.DMA((2, 2, 2)),
                pltpu.SemaphoreType.DMA((2,)),
                pltpu.SemaphoreType.DMA((2,)),
            ],
            compiler_params=pltpu.CompilerParams(has_side_effects=True),
        )(velocity, pressure, force, viscosity, element_stiffness, element_divergence,
          jnp.asarray(row_map))

    spec = P(None, "patch", None, "shell")
    return jax.shard_map(
        per_device,
        mesh=mesh,
        in_specs=(spec, spec, spec, P("patch", None, "shell"), P(), P()),
        out_specs=(spec, spec),
        check_vma=False,
    )
```

```python
import functools

import jax
import jax.numpy as jnp
import numpy as np
from jax import lax
from jax.experimental import pallas as pl
from jax.experimental.pallas import tpu as pltpu
from jax.sharding import PartitionSpec as P

ITERS = 2
MESH = pl.DeviceIdType.MESH
SLOTS = 16
F32 = jnp.float32
BF16 = jnp.bfloat16


def unknown_map():
    rows = np.zeros((9 * SLOTS, 81), np.float32)
    for x in range(3):
        for a in range(3):
            for b in range(3):
                for c in range(3):
                    rows[(b * 3 + a) * SLOTS + c * 3 + x, x * 27 + a * 9 + b * 3 + c] = 1.0
    return rows


def dot(x, y, contract=((1,), (0,))):
    return lax.dot_general(x, y, (contract, ((), ())), preferred_element_type=F32)


def split2(x):
    hi = x.astype(BF16)
    return hi, (x - hi.astype(F32)).astype(BF16)


def exact_dot(x, perm):
    hi, mid = split2(x)
    lo = (x - hi.astype(F32) - mid.astype(F32)).astype(BF16)
    return dot(hi, perm) + dot(mid, perm) + dot(lo, perm)


def kernel(
    dims,
    v_hbm, p_hbm, f_hbm, visc_hbm, stiff_hbm, div_hbm, map_hbm,
    sol_ref, pout_ref,
    v_ref, p_ref, f_ref, visc_ref, stiff_ref, div_ref, map_ref, in_sems,
    fld, fhi, flo, out, out2, pq, bvals,
    vplane, vcol, vcol_in, vdiag_in,
    col_out, col_in, plane_out, plane_in, sums,
    bar_send, bar_recv, ex_send, ex_recv, ar_send, ar_recv,
):
    n_patch, n_shell, ea, eb, na, nb, lanes = dims
    n_dev = n_patch * n_shell
    planes = na + 1
    block = 3 * nb
    owned = na * block
    rows = planes * block
    width = vcol.shape[1]
    stride = planes * SLOTS
    patch = lax.axis_index("patch")
    shell = lax.axis_index("shell")
    after = lax.rem(patch + 1, n_patch)
    before = lax.rem(patch + n_patch - 1, n_patch)
    has_above = shell < n_shell - 1
    has_below = shell > 0
    above = jnp.minimum(shell + 1, n_shell - 1)
    below = jnp.maximum(shell - 1, 0)

    def remote(src, dst, send, recv, to_patch, to_shell):
        return pltpu.make_async_remote_copy(
            src_ref=src, dst_ref=dst, send_sem=send, recv_sem=recv,
            device_id={"patch": to_patch, "shell": to_shell}, device_id_type=MESH,
        )

    loads = [
        pltpu.make_async_copy(source, target, in_sems.at[k])
        for k, (source, target) in enumerate((
            (v_hbm, v_ref), (stiff_hbm, stiff_ref), (div_hbm, div_ref), (map_hbm, map_ref),
            (f_hbm, f_ref), (p_hbm, p_ref), (visc_hbm, visc_ref)))
    ]
    for load in loads:
        load.start()
    barrier = pltpu.get_barrier_semaphore()

    @pl.loop(1, n_dev)
    def _(d):
        to = lax.rem(patch * n_shell + shell + d, n_dev)
        pl.semaphore_signal(
            barrier, inc=1, device_id_type=MESH,
            device_id={"patch": lax.div(to, n_shell), "shell": lax.rem(to, n_shell)})

    @pl.when(jnp.logical_not(has_above))
    def _():
        col_in[2] = jnp.zeros(col_in.shape[1:], F32)
        vcol_in[...] = jnp.zeros_like(vcol_in)
        vdiag_in[...] = jnp.zeros_like(vdiag_in)

    @pl.when(jnp.logical_not(has_below))
    def _():
        col_in[1] = jnp.zeros(col_in.shape[1:], F32)

    fld[...] = jnp.zeros_like(fld)
    pq[...] = jnp.zeros_like(pq)
    out[...] = jnp.zeros_like(out)
    out2[...] = jnp.zeros_like(out2)
    for load in loads:
        load.wait()
    plane_copy = remote(v_hbm.at[:, 0], vplane, bar_send.at[0], bar_recv.at[0], before, shell)
    head = jnp.concatenate(
        [v_ref[x, a, :, :lanes] for a in range(na) for x in range(3)]
        + [jnp.zeros((width - owned, lanes), F32)], axis=0)
    vcol[...] = jnp.transpose(head)[:8]
    col_copy = remote(vcol, vcol_in, bar_send.at[1], bar_recv.at[1], patch, below)
    diag_copy = remote(vcol, vdiag_in, bar_send.at[2], bar_recv.at[2], before, below)

    row_map = map_ref[...].astype(BF16)
    a_hi, a_lo = split2(stiff_ref[...])
    div = jnp.concatenate([div_ref[...], jnp.zeros((4, 81), F32)], axis=0)
    b_hi = div.astype(BF16).astype(F32)
    b_lo = (div - b_hi).astype(BF16).astype(F32)

    def both_sides(mat):
        return dot(dot(row_map, mat).astype(BF16), row_map, ((1,), (1,)))

    def right_side(mat):
        return dot(mat.astype(BF16), row_map, ((1,), (1,)))

    apply_hi = jnp.concatenate([both_sides(a_hi), right_side(b_hi)], axis=0).astype(BF16)
    apply_lo = jnp.concatenate([both_sides(a_lo), right_side(b_lo)], axis=0).astype(BF16)
    apply_all = jnp.concatenate([apply_hi, apply_lo], axis=0)
    b_stack = jnp.concatenate([b_hi, b_lo, b_hi, jnp.zeros((8, 81), F32)], axis=0).astype(BF16)
    back = dot(row_map, b_stack, ((1,), (1,))).astype(BF16)
    m_rows = 9 * SLOTS
    span = 3 * SLOTS

    r_i = lax.broadcasted_iota(jnp.int32, (2 * lanes, 2 * lanes), 0)
    c_i = lax.broadcasted_iota(jnp.int32, (2 * lanes, 2 * lanes), 1)
    unzip = (r_i == jnp.where(c_i < lanes, 2 * c_i, 2 * c_i - 2 * lanes + 1)).astype(BF16)
    rezip = (c_i == jnp.where(r_i < lanes, 2 * r_i, 2 * r_i - 2 * lanes + 1)).astype(BF16)

    for i in range(ea):
        for q in range(4):
            pq[pl.ds(i * eb * 8 + q, eb, stride=8), :] = p_ref[q, i]
    inv_visc = [1.0 / visc_ref[i] for i in range(ea)]
    visc = [visc_ref[i] for i in range(ea)]

    f_n = exact_dot(jnp.concatenate(
        [f_ref[x, a] for a in range(na) for x in range(3)], axis=0), unzip)
    zero_plane = jnp.zeros((block, lanes), F32)
    f_e = jnp.concatenate([f_n[:, :lanes], zero_plane], axis=0)
    f_o = jnp.concatenate([f_n[:, lanes:], zero_plane], axis=0)
    v_own = exact_dot(jnp.concatenate(
        [v_ref[x, a] for a in range(na) for x in range(3)], axis=0), unzip)

    pl.semaphore_wait(barrier, n_dev - 1)
    plane_copy.start()

    @pl.when(has_below)
    def _():
        col_copy.start()
        diag_copy.start()

    lane_n = lax.broadcasted_iota(jnp.int32, (rows, lanes), 1)
    col_lane = lax.broadcasted_iota(jnp.int32, (1, width), 1)

    def column(row):
        return jnp.transpose(jnp.broadcast_to(row, (lanes, width)))[:rows]

    def put(even, odd, ghost):
        shifted = pltpu.roll(jnp.where(lane_n == 0, column(ghost), even), lanes - 1, 1)
        for a in range(planes):
            for x in range(3):
                at = (a * 3 + x) * nb
                for c, part in ((0, even), (1, odd), (2, shifted)):
                    fld[pl.ds(a * SLOTS + c * 3 + x, nb, stride=stride), :] = part[at:at + nb]
        hi, lo = split2(fld[...])
        fhi[...] = hi
        flo[...] = lo

    def gathered(ref, j):
        parts = []
        for i in range(ea):
            parts.append(jnp.concatenate(
                [ref[(2 * j + b) * stride + 2 * i * SLOTS:(2 * j + b) * stride + 2 * i * SLOTS + span]
                 for b in range(3)], axis=0))
        return jnp.concatenate(parts, axis=1)

    def back_apply(pieces):
        packed = []
        for w in pieces:
            hi = w.astype(BF16).astype(F32)
            packed.append(jnp.concatenate([hi, hi, w - hi, jnp.zeros_like(w)], axis=0))
        return dot(back, jnp.concatenate(packed, axis=1).astype(BF16))

    def add_to(ref, terms, i, j):
        for b in range(3):
            at = (2 * j + b) * stride + 2 * i * SLOTS
            ref[at:at + span] = ref[at:at + span] + terms[b * span:(b + 1) * span]

    def operator(mode, slot):
        if mode == "second":
            out[...] = jnp.zeros_like(out)
        energy = jnp.zeros((8, lanes), F32)
        full = None
        for step in range(eb + 1):
            ready = full
            if step < eb:
                hi = dot(apply_all, gathered(fhi, step))
                full = hi[:m_rows + 8] + hi[m_rows + 8:] + dot(apply_hi, gathered(flo, step))
            if step == 0:
                continue
            j = step - 1
            scaled = []
            for i in range(ea):
                bv = ready[m_rows:, i * lanes:(i + 1) * lanes]
                at = (i * eb + j) * 8
                bvals[slot, at:at + 8] = bv
                if mode == "first":
                    scaled.append(pq[at:at + 8])
                else:
                    scaled.append(bv * inv_visc[i][j:j + 1])
            if mode != "last":
                extra = back_apply(scaled)
            for i in range(ea):
                terms = ready[:m_rows, i * lanes:(i + 1) * lanes] * visc[i][j:j + 1]
                if mode != "first":
                    vals = jnp.concatenate(
                        [fld[(2 * j + b) * stride + 2 * i * SLOTS:
                             (2 * j + b) * stride + 2 * i * SLOTS + span] for b in range(3)], axis=0)
                    energy = energy + jnp.sum((terms * vals).reshape(m_rows // 8, 8, lanes), axis=0)
                if mode != "last":
                    add_to(out, terms + extra[:, i * lanes:(i + 1) * lanes], i, j)
        return energy

    def pressure_change():
        for j in range(eb):
            extra = back_apply(
                [bvals[0, (i * eb + j) * 8:(i * eb + j) * 8 + 8] * inv_visc[i][j:j + 1]
                 for i in range(ea)])
            for i in range(ea):
                add_to(out2, extra[:, i * lanes:(i + 1) * lanes], i, j)

    def collect(ref, c):
        return jnp.concatenate(
            [ref[pl.ds(a * SLOTS + c * 3 + x, nb, stride=stride), :]
             for a in range(planes) for x in range(3)], axis=0)

    def padded(part):
        return jnp.concatenate([part, jnp.zeros((width - rows, lanes), F32)], axis=0)

    def stage(n, even, odd, carry):
        even = even + pltpu.roll(jnp.where(lane_n == lanes - 1, 0.0, carry), 1, 1)
        high = jnp.transpose(padded(carry))[lanes - 8:][7:8]
        col_out[0, n] = high
        col_out[1, n] = jnp.transpose(padded(even))[:8][0:1]
        for side, at in ((0, 0), (1, owned)):
            plane_out[side, n, 0] = even[at:at + block]
            plane_out[side, n, 1] = odd[at:at + block]
        flat, up, down = [], [], []

        def message(group, source, target, k, to_patch, to_shell):
            group.append(remote(source, target, ex_send.at[n, k], ex_recv.at[n, k],
                                to_patch, to_shell))

        message(flat, plane_out.at[0, n], plane_in.at[0, n], 0, before, shell)
        message(flat, plane_out.at[1, n], plane_in.at[1, n], 1, after, shell)
        for src, to in ((1, after), (2, before)):
            message(flat, col_out.at[0, n], col_in.at[0, n, src], 1 + src, to, shell)
        for src, to in ((0, patch), (1, after), (2, before)):
            message(up, col_out.at[0, n], col_in.at[1, n, src], 4 + src, to, above)
            message(down, col_out.at[1, n], col_in.at[2, n, src], 7 + src, to, below)
        return even, odd, high, (flat, up, down)

    def begin(staged):
        flat, up, down = staged[3]

        @pl.when(has_above)
        def _():
            for copy in up:
                copy.start()

        @pl.when(has_below)
        def _():
            for copy in down:
                copy.start()

        for copy in flat[2:] + flat[:2]:
            copy.start()

    def complete(n, staged):
        even, odd, high, (flat, up, down) = staged

        @pl.when(has_above)
        def _():
            for copy in down:
                copy.wait_recv()
            for copy in up:
                copy.wait_send()

        @pl.when(has_below)
        def _():
            for copy in up:
                copy.wait_recv()
            for copy in down:
                copy.wait_send()

        for copy in flat:
            copy.wait()

        def joined_row(own, kind):
            prev = jnp.broadcast_to(col_in[kind, n, 1], (8, width))
            nxt = jnp.broadcast_to(col_in[kind, n, 2], (8, width))
            row = own + jnp.where(col_lane < block, pltpu.roll(prev, width - owned, 1)[0:1], 0.0)
            return row + jnp.where(
                jnp.logical_and(col_lane >= owned, col_lane < rows),
                pltpu.roll(nxt, owned, 1)[0:1], 0.0)

        def joined(part, k):
            return jnp.concatenate(
                [part[:block] + plane_in[1, n, k], part[block:owned],
                 part[owned:] + plane_in[0, n, k]], axis=0)

        ghost = jnp.where(
            has_above, joined_row(high, 0) + joined_row(col_in[2, n, 0], 2), 0.0)
        from_below = column(joined_row(col_in[1, n, 0], 1))
        return (joined(even, 0) + jnp.where(lane_n == 0, from_below, 0.0), joined(odd, 1), ghost)

    me = patch * n_shell + shell

    def norm_of(even, odd):
        sq = even[:owned] * even[:owned] + odd[:owned] * odd[:owned]
        return jnp.sum(sq.reshape(owned // 8, 8, lanes), axis=0)

    def sums_start(phase, norm, energy):
        sums[phase, me] = jnp.concatenate(
            [jnp.sum(norm, axis=0, keepdims=True), jnp.sum(energy, axis=0, keepdims=True)], axis=0)

        @pl.loop(1, n_dev)
        def _(d):
            to = lax.rem(me + d, n_dev)
            remote(sums.at[phase, me], sums.at[phase, me], ar_send.at[phase], ar_recv.at[phase],
                   lax.div(to, n_shell), lax.rem(to, n_shell)).start()

    def sums_end(phase):
        whole = sums.at[phase, pl.ds(0, n_dev - 1)]
        pltpu.make_async_copy(whole, whole, ar_send.at[phase]).wait()
        pltpu.make_async_copy(whole, whole, ar_recv.at[phase]).wait()
        total = jnp.sum(sums[phase], axis=0)
        total = jnp.sum(total, axis=1, keepdims=True)
        return total[0:1] / total[1:2]

    plane_copy.wait()

    @pl.when(has_below)
    def _():
        col_copy.wait_send()
        diag_copy.wait_send()

    @pl.when(has_above)
    def _():
        col_copy.wait_recv()
        diag_copy.wait_recv()

    v_next = exact_dot(jnp.concatenate([vplane[x] for x in range(3)], axis=0), unzip)
    v_e = jnp.concatenate([v_own[:, :lanes], v_next[:, :lanes]], axis=0)
    v_o = jnp.concatenate([v_own[:, lanes:], v_next[:, lanes:]], axis=0)
    v_g = jnp.where(col_lane < owned, vcol_in[0:1], pltpu.roll(vdiag_in[...], owned, 1)[0:1])
    put(v_e, v_o, v_g)

    operator("first", 0)
    sent = stage(0, f_e - collect(out, 0), f_o - collect(out, 1), -collect(out, 2))
    begin(sent)
    pressure_change()
    sent_change = stage(1, *[collect(out2, c) for c in range(3)])
    r0 = complete(0, sent)
    begin(sent_change)
    put(*r0)
    energy = operator("second", 1)
    sums_start(0, norm_of(r0[0], r0[1]), energy)
    sent = stage(2, *[collect(out, c) for c in range(3)])
    begin(sent)
    change = complete(1, sent_change)
    base = [x - y for x, y in zip(r0, change)]
    h0 = complete(2, sent)
    step0 = sums_end(0)
    r1 = tuple(s - step0 * h for s, h in zip(base, h0))
    put(*r1)
    energy = operator("last", 2)
    sums_start(1, norm_of(r1[0], r1[1]), energy)
    part_e = (v_e + step0 * r0[0])[:owned]
    part_o = (v_o + step0 * r0[1])[:owned]
    step1 = sums_end(1)
    result = exact_dot(jnp.concatenate(
        [part_e + step1 * r1[0][:owned], part_o + step1 * r1[1][:owned]], axis=1), rezip)
    for a in range(na):
        for x in range(3):
            at = (a * 3 + x) * nb
            sol_ref[x, a] = result[at:at + nb]
    bvals[0] = 2.0 * (bvals[0] + step0 * bvals[1]) + step1 * bvals[2]
    for i in range(ea):
        for q in range(4):
            pout_ref[q, i] = p_ref[q, i] + bvals[0, pl.ds(i * eb * 8 + q, eb, stride=8), :] * inv_visc[i]


def solution(mesh):
    n_patch, n_shell = mesh.shape["patch"], mesh.shape["shell"]
    row_map = unknown_map()

    def per_device(velocity, pressure, force, viscosity, element_stiffness, element_divergence):
        ea, eb, lanes = viscosity.shape
        na, nb = velocity.shape[1], velocity.shape[2]
        dims = (n_patch, n_shell, ea, eb, na, nb, lanes)
        block = 3 * nb
        width = -(-(na + 1) * block // 128) * 128
        g_rows = (nb + 1) * (na + 1) * SLOTS
        vmem = pl.BlockSpec(memory_space=pltpu.VMEM)
        return pl.pallas_call(
            functools.partial(kernel, dims),
            out_shape=(jax.ShapeDtypeStruct(velocity.shape, F32),
                       jax.ShapeDtypeStruct(pressure.shape, F32)),
            in_specs=[pl.BlockSpec(memory_space=pl.ANY)] * 7,
            out_specs=(vmem, vmem),
            scratch_shapes=[
                pltpu.VMEM(velocity.shape, F32),
                pltpu.VMEM(pressure.shape, F32),
                pltpu.VMEM(force.shape, F32),
                pltpu.VMEM(viscosity.shape, F32),
                pltpu.VMEM(element_stiffness.shape, F32),
                pltpu.VMEM(element_divergence.shape, F32),
                pltpu.VMEM(row_map.shape, F32),
                pltpu.SemaphoreType.DMA((7,)),
                pltpu.VMEM((g_rows, lanes), F32),
                pltpu.VMEM((g_rows, lanes), BF16),
                pltpu.VMEM((g_rows, lanes), BF16),
                pltpu.VMEM((g_rows, lanes), F32),
                pltpu.VMEM((g_rows, lanes), F32),
                pltpu.VMEM((ea * eb * 8, lanes), F32),
                pltpu.VMEM((3, ea * eb * 8, lanes), F32),
                pltpu.VMEM((3, nb, 2 * lanes), F32),
                pltpu.VMEM((8, width), F32),
                pltpu.VMEM((8, width), F32),
                pltpu.VMEM((8, width), F32),
                pltpu.VMEM((2, 3, 1, width), F32),
                pltpu.VMEM((3, 3, 3, 1, width), F32),
                pltpu.VMEM((2, 3, 2, block, lanes), F32),
                pltpu.VMEM((2, 3, 2, block, lanes), F32),
                pltpu.VMEM((2, n_patch * n_shell, 2, lanes), F32),
                pltpu.SemaphoreType.DMA((3,)),
                pltpu.SemaphoreType.DMA((3,)),
                pltpu.SemaphoreType.DMA((3, 10)),
                pltpu.SemaphoreType.DMA((3, 10)),
                pltpu.SemaphoreType.DMA((2,)),
                pltpu.SemaphoreType.DMA((2,)),
            ],
            compiler_params=pltpu.CompilerParams(collective_id=0, has_side_effects=True),
        )(velocity, pressure, force, viscosity, element_stiffness, element_divergence,
          jnp.asarray(row_map))

    spec = P(None, "patch", None, "shell")
    return jax.shard_map(
        per_device,
        mesh=mesh,
        in_specs=(spec, spec, spec, P("patch", None, "shell"), P(), P()),
        out_specs=(spec, spec),
        check_vma=False,
    )
```

```python
import functools

import jax
import jax.numpy as jnp
import numpy as np
from jax import lax
from jax.experimental import pallas as pl
from jax.experimental.pallas import tpu as pltpu
from jax.sharding import PartitionSpec as P

ITERS = 2
MESH = pl.DeviceIdType.MESH
SLOTS = 16
F32 = jnp.float32
BF16 = jnp.bfloat16


def unknown_map():
    rows = np.zeros((9 * SLOTS, 81), np.float32)
    for x in range(3):
        for a in range(3):
            for b in range(3):
                for c in range(3):
                    rows[(b * 3 + a) * SLOTS + c * 3 + x, x * 27 + a * 9 + b * 3 + c] = 1.0
    return rows


def dot(x, y, contract=((1,), (0,))):
    return lax.dot_general(x, y, (contract, ((), ())), preferred_element_type=F32)


def split2(x):
    hi = x.astype(BF16)
    return hi, (x - hi.astype(F32)).astype(BF16)


def exact_dot(x, perm):
    hi, mid = split2(x)
    lo = (x - hi.astype(F32) - mid.astype(F32)).astype(BF16)
    return dot(hi, perm) + dot(mid, perm) + dot(lo, perm)


def kernel(
    dims,
    v_hbm, p_hbm, f_hbm, visc_hbm, stiff_hbm, div_hbm, map_hbm,
    sol_ref, pout_ref,
    v_ref, p_ref, f_ref, visc_ref, stiff_ref, div_ref, map_ref, in_sems,
    fld, fhi, flo, out, out2, pq, bvals,
    vplane, vcol, vcol_in, vdiag_in,
    col_out, col_in, plane_out, plane_in, sums, far_sums,
    bar_send, bar_recv, ex_send, ex_recv, ar_send, ar_recv,
):
    n_patch, n_shell, ea, eb, na, nb, lanes = dims
    n_dev = n_patch * n_shell
    planes = na + 1
    block = 3 * nb
    owned = na * block
    rows = planes * block
    width = vcol.shape[1]
    stride = planes * SLOTS
    patch = lax.axis_index("patch")
    shell = lax.axis_index("shell")
    after = lax.rem(patch + 1, n_patch)
    before = lax.rem(patch + n_patch - 1, n_patch)
    has_above = shell < n_shell - 1
    has_below = shell > 0
    above = jnp.minimum(shell + 1, n_shell - 1)
    below = jnp.maximum(shell - 1, 0)

    def remote(src, dst, send, recv, to_patch, to_shell):
        return pltpu.make_async_remote_copy(
            src_ref=src, dst_ref=dst, send_sem=send, recv_sem=recv,
            device_id={"patch": to_patch, "shell": to_shell}, device_id_type=MESH,
        )

    loads = [
        pltpu.make_async_copy(source, target, in_sems.at[k])
        for k, (source, target) in enumerate((
            (v_hbm, v_ref), (stiff_hbm, stiff_ref), (div_hbm, div_ref), (map_hbm, map_ref),
            (f_hbm, f_ref), (p_hbm, p_ref), (visc_hbm, visc_ref)))
    ]
    for load in loads:
        load.start()
    barrier = pltpu.get_barrier_semaphore()

    @pl.loop(1, n_dev)
    def _(d):
        to = lax.rem(patch * n_shell + shell + d, n_dev)
        pl.semaphore_signal(
            barrier, inc=1, device_id_type=MESH,
            device_id={"patch": lax.div(to, n_shell), "shell": lax.rem(to, n_shell)})

    @pl.when(jnp.logical_not(has_above))
    def _():
        col_in[2] = jnp.zeros(col_in.shape[1:], F32)
        vcol_in[...] = jnp.zeros_like(vcol_in)
        vdiag_in[...] = jnp.zeros_like(vdiag_in)

    @pl.when(jnp.logical_not(has_below))
    def _():
        col_in[1] = jnp.zeros(col_in.shape[1:], F32)

    fld[...] = jnp.zeros_like(fld)
    pq[...] = jnp.zeros_like(pq)
    out[...] = jnp.zeros_like(out)
    out2[...] = jnp.zeros_like(out2)
    for load in loads:
        load.wait()
    plane_copy = remote(v_hbm.at[:, 0], vplane, bar_send.at[0], bar_recv.at[0], before, shell)
    head = jnp.concatenate(
        [v_ref[x, a, :, :lanes] for a in range(na) for x in range(3)]
        + [jnp.zeros((width - owned, lanes), F32)], axis=0)
    vcol[...] = jnp.transpose(head)[:8]
    col_copy = remote(vcol, vcol_in, bar_send.at[1], bar_recv.at[1], patch, below)
    diag_copy = remote(vcol, vdiag_in, bar_send.at[2], bar_recv.at[2], before, below)

    row_map = map_ref[...].astype(BF16)
    a_hi, a_lo = split2(stiff_ref[...])
    div = jnp.concatenate([div_ref[...], jnp.zeros((4, 81), F32)], axis=0)
    b_hi = div.astype(BF16).astype(F32)
    b_lo = (div - b_hi).astype(BF16).astype(F32)

    def both_sides(mat):
        return dot(dot(row_map, mat).astype(BF16), row_map, ((1,), (1,)))

    def right_side(mat):
        return dot(mat.astype(BF16), row_map, ((1,), (1,)))

    apply_hi = jnp.concatenate([both_sides(a_hi), right_side(b_hi)], axis=0).astype(BF16)
    apply_lo = jnp.concatenate([both_sides(a_lo), right_side(b_lo)], axis=0).astype(BF16)
    apply_all = jnp.concatenate([apply_hi, apply_lo], axis=0)
    b_stack = jnp.concatenate([b_hi, b_lo, b_hi, jnp.zeros((8, 81), F32)], axis=0).astype(BF16)
    back = dot(row_map, b_stack, ((1,), (1,))).astype(BF16)
    m_rows = 9 * SLOTS
    span = 3 * SLOTS

    r_i = lax.broadcasted_iota(jnp.int32, (2 * lanes, 2 * lanes), 0)
    c_i = lax.broadcasted_iota(jnp.int32, (2 * lanes, 2 * lanes), 1)
    unzip = (r_i == jnp.where(c_i < lanes, 2 * c_i, 2 * c_i - 2 * lanes + 1)).astype(BF16)
    rezip = (c_i == jnp.where(r_i < lanes, 2 * r_i, 2 * r_i - 2 * lanes + 1)).astype(BF16)

    for i in range(ea):
        for q in range(4):
            pq[pl.ds(i * eb * 8 + q, eb, stride=8), :] = p_ref[q, i]
    inv_visc = [1.0 / visc_ref[i] for i in range(ea)]
    visc = [visc_ref[i] for i in range(ea)]

    f_n = exact_dot(jnp.concatenate(
        [f_ref[x, a] for a in range(na) for x in range(3)], axis=0), unzip)
    zero_plane = jnp.zeros((block, lanes), F32)
    f_e = jnp.concatenate([f_n[:, :lanes], zero_plane], axis=0)
    f_o = jnp.concatenate([f_n[:, lanes:], zero_plane], axis=0)
    v_own = exact_dot(jnp.concatenate(
        [v_ref[x, a] for a in range(na) for x in range(3)], axis=0), unzip)

    pl.semaphore_wait(barrier, n_dev - 1)
    plane_copy.start()

    @pl.when(has_below)
    def _():
        col_copy.start()
        diag_copy.start()

    lane_n = lax.broadcasted_iota(jnp.int32, (rows, lanes), 1)
    col_lane = lax.broadcasted_iota(jnp.int32, (1, width), 1)

    def column(row):
        return jnp.transpose(jnp.broadcast_to(row, (lanes, width)))[:rows]

    def put(even, odd, ghost):
        shifted = pltpu.roll(jnp.where(lane_n == 0, column(ghost), even), lanes - 1, 1)
        for a in range(planes):
            for x in range(3):
                at = (a * 3 + x) * nb
                for c, part in ((0, even), (1, odd), (2, shifted)):
                    fld[pl.ds(a * SLOTS + c * 3 + x, nb, stride=stride), :] = part[at:at + nb]
        hi, lo = split2(fld[...])
        fhi[...] = hi
        flo[...] = lo

    def gathered(ref, j):
        parts = []
        for i in range(ea):
            parts.append(jnp.concatenate(
                [ref[(2 * j + b) * stride + 2 * i * SLOTS:(2 * j + b) * stride + 2 * i * SLOTS + span]
                 for b in range(3)], axis=0))
        return jnp.concatenate(parts, axis=1)

    def back_apply(pieces):
        packed = []
        for w in pieces:
            hi = w.astype(BF16).astype(F32)
            packed.append(jnp.concatenate([hi, hi, w - hi, jnp.zeros_like(w)], axis=0))
        return dot(back, jnp.concatenate(packed, axis=1).astype(BF16))

    def add_to(ref, terms, i, j):
        for b in range(3):
            at = (2 * j + b) * stride + 2 * i * SLOTS
            ref[at:at + span] = ref[at:at + span] + terms[b * span:(b + 1) * span]

    def operator(mode, slot):
        if mode == "second":
            out[...] = jnp.zeros_like(out)
        energy = jnp.zeros((8, lanes), F32)
        full = None
        for step in range(eb + 1):
            ready = full
            if step < eb:
                hi = dot(apply_all, gathered(fhi, step))
                full = hi[:m_rows + 8] + hi[m_rows + 8:] + dot(apply_hi, gathered(flo, step))
            if step == 0:
                continue
            j = step - 1
            scaled = []
            for i in range(ea):
                bv = ready[m_rows:, i * lanes:(i + 1) * lanes]
                at = (i * eb + j) * 8
                bvals[slot, at:at + 8] = bv
                if mode == "first":
                    scaled.append(pq[at:at + 8])
                else:
                    scaled.append(bv * inv_visc[i][j:j + 1])
            if mode != "last":
                extra = back_apply(scaled)
            for i in range(ea):
                terms = ready[:m_rows, i * lanes:(i + 1) * lanes] * visc[i][j:j + 1]
                if mode != "first":
                    vals = jnp.concatenate(
                        [fld[(2 * j + b) * stride + 2 * i * SLOTS:
                             (2 * j + b) * stride + 2 * i * SLOTS + span] for b in range(3)], axis=0)
                    energy = energy + jnp.sum((terms * vals).reshape(m_rows // 8, 8, lanes), axis=0)
                if mode != "last":
                    add_to(out, terms + extra[:, i * lanes:(i + 1) * lanes], i, j)
        return energy

    def pressure_change():
        for j in range(eb):
            extra = back_apply(
                [bvals[0, (i * eb + j) * 8:(i * eb + j) * 8 + 8] * inv_visc[i][j:j + 1]
                 for i in range(ea)])
            for i in range(ea):
                add_to(out2, extra[:, i * lanes:(i + 1) * lanes], i, j)

    def collect(ref, c):
        return jnp.concatenate(
            [ref[pl.ds(a * SLOTS + c * 3 + x, nb, stride=stride), :]
             for a in range(planes) for x in range(3)], axis=0)

    def padded(part):
        return jnp.concatenate([part, jnp.zeros((width - rows, lanes), F32)], axis=0)

    def stage(n, even, odd, carry):
        even = even + pltpu.roll(jnp.where(lane_n == lanes - 1, 0.0, carry), 1, 1)
        high = jnp.transpose(padded(carry))[lanes - 8:][7:8]
        col_out[0, n] = high
        col_out[1, n] = jnp.transpose(padded(even))[:8][0:1]
        for side, at in ((0, 0), (1, owned)):
            plane_out[side, n, 0] = even[at:at + block]
            plane_out[side, n, 1] = odd[at:at + block]
        flat, up, down = [], [], []

        def message(group, source, target, k, to_patch, to_shell):
            group.append(remote(source, target, ex_send.at[n, k], ex_recv.at[n, k],
                                to_patch, to_shell))

        message(flat, plane_out.at[0, n], plane_in.at[0, n], 0, before, shell)
        message(flat, plane_out.at[1, n], plane_in.at[1, n], 1, after, shell)
        for src, to in ((1, after), (2, before)):
            message(flat, col_out.at[0, n], col_in.at[0, n, src], 1 + src, to, shell)
        for src, to in ((0, patch), (1, after), (2, before)):
            message(up, col_out.at[0, n], col_in.at[1, n, src], 4 + src, to, above)
            message(down, col_out.at[1, n], col_in.at[2, n, src], 7 + src, to, below)
        return even, odd, high, (flat, up, down)

    def begin(staged):
        flat, up, down = staged[3]

        @pl.when(has_above)
        def _():
            for copy in up:
                copy.start()

        @pl.when(has_below)
        def _():
            for copy in down:
                copy.start()

        for copy in flat[2:] + flat[:2]:
            copy.start()

    def complete(n, staged):
        even, odd, high, (flat, up, down) = staged

        @pl.when(has_above)
        def _():
            for copy in down:
                copy.wait_recv()
            for copy in up:
                copy.wait_send()

        @pl.when(has_below)
        def _():
            for copy in up:
                copy.wait_recv()
            for copy in down:
                copy.wait_send()

        for copy in flat:
            copy.wait()

        def joined_row(own, kind):
            prev = jnp.broadcast_to(col_in[kind, n, 1], (8, width))
            nxt = jnp.broadcast_to(col_in[kind, n, 2], (8, width))
            row = own + jnp.where(col_lane < block, pltpu.roll(prev, width - owned, 1)[0:1], 0.0)
            return row + jnp.where(
                jnp.logical_and(col_lane >= owned, col_lane < rows),
                pltpu.roll(nxt, owned, 1)[0:1], 0.0)

        def joined(part, k):
            return jnp.concatenate(
                [part[:block] + plane_in[1, n, k], part[block:owned],
                 part[owned:] + plane_in[0, n, k]], axis=0)

        ghost = jnp.where(
            has_above, joined_row(high, 0) + joined_row(col_in[2, n, 0], 2), 0.0)
        from_below = column(joined_row(col_in[1, n, 0], 1))
        return (joined(even, 0) + jnp.where(lane_n == 0, from_below, 0.0), joined(odd, 1), ghost)

    inner = max(k for k in range(1, n_patch + 1) if k * k <= n_patch and n_patch % k == 0)
    n_near, n_far = inner * n_shell, n_patch // inner
    group = lax.div(patch, inner)
    near = lax.rem(patch, inner) * n_shell + shell

    def norm_of(even, odd):
        sq = even[:owned] * even[:owned] + odd[:owned] * odd[:owned]
        return jnp.sum(sq.reshape(owned // 8, 8, lanes), axis=0)

    def sums_start(phase, norm, energy):
        sums[phase, near] = jnp.concatenate(
            [jnp.sum(norm, axis=0, keepdims=True), jnp.sum(energy, axis=0, keepdims=True)], axis=0)

        @pl.loop(1, n_near)
        def _(d):
            to = lax.rem(near + d, n_near)
            remote(sums.at[phase, near], sums.at[phase, near],
                   ar_send.at[phase, 0], ar_recv.at[phase, 0],
                   group * inner + lax.div(to, n_shell), lax.rem(to, n_shell)).start()

    def settle(buffer, count, phase, level):
        if count > 1:
            whole = buffer.at[phase, pl.ds(0, count - 1)]
            pltpu.make_async_copy(whole, whole, ar_send.at[phase, level]).wait()
            pltpu.make_async_copy(whole, whole, ar_recv.at[phase, level]).wait()
        return jnp.sum(buffer[phase], axis=0)

    def sums_middle(phase):
        far_sums[phase, group] = settle(sums, n_near, phase, 0)

        @pl.loop(1, n_far)
        def _(d):
            to = lax.rem(group + d, n_far)
            remote(far_sums.at[phase, group], far_sums.at[phase, group],
                   ar_send.at[phase, 1], ar_recv.at[phase, 1],
                   to * inner + lax.rem(patch, inner), shell).start()

    def sums_end(phase):
        total = jnp.sum(settle(far_sums, n_far, phase, 1), axis=1, keepdims=True)
        return total[0:1] / total[1:2]

    plane_copy.wait()

    @pl.when(has_below)
    def _():
        col_copy.wait_send()
        diag_copy.wait_send()

    @pl.when(has_above)
    def _():
        col_copy.wait_recv()
        diag_copy.wait_recv()

    v_next = exact_dot(jnp.concatenate([vplane[x] for x in range(3)], axis=0), unzip)
    v_e = jnp.concatenate([v_own[:, :lanes], v_next[:, :lanes]], axis=0)
    v_o = jnp.concatenate([v_own[:, lanes:], v_next[:, lanes:]], axis=0)
    v_g = jnp.where(col_lane < owned, vcol_in[0:1], pltpu.roll(vdiag_in[...], owned, 1)[0:1])
    put(v_e, v_o, v_g)

    operator("first", 0)
    sent = stage(0, f_e - collect(out, 0), f_o - collect(out, 1), -collect(out, 2))
    begin(sent)
    pressure_change()
    sent_change = stage(1, *[collect(out2, c) for c in range(3)])
    r0 = complete(0, sent)
    begin(sent_change)
    put(*r0)
    energy = operator("second", 1)
    sums_start(0, norm_of(r0[0], r0[1]), energy)
    sent = stage(2, *[collect(out, c) for c in range(3)])
    begin(sent)
    change = complete(1, sent_change)
    base = [x - y for x, y in zip(r0, change)]
    sums_middle(0)
    h0 = complete(2, sent)
    step0 = sums_end(0)
    r1 = tuple(s - step0 * h for s, h in zip(base, h0))
    put(*r1)
    energy = operator("last", 2)
    sums_start(1, norm_of(r1[0], r1[1]), energy)
    part_e = (v_e + step0 * r0[0])[:owned]
    part_o = (v_o + step0 * r0[1])[:owned]
    sums_middle(1)
    step1 = sums_end(1)
    result = exact_dot(jnp.concatenate(
        [part_e + step1 * r1[0][:owned], part_o + step1 * r1[1][:owned]], axis=1), rezip)
    for a in range(na):
        for x in range(3):
            at = (a * 3 + x) * nb
            sol_ref[x, a] = result[at:at + nb]
    bvals[0] = 2.0 * (bvals[0] + step0 * bvals[1]) + step1 * bvals[2]
    for i in range(ea):
        for q in range(4):
            pout_ref[q, i] = p_ref[q, i] + bvals[0, pl.ds(i * eb * 8 + q, eb, stride=8), :] * inv_visc[i]


def solution(mesh):
    n_patch, n_shell = mesh.shape["patch"], mesh.shape["shell"]
    row_map = unknown_map()
    inner = max(k for k in range(1, n_patch + 1) if k * k <= n_patch and n_patch % k == 0)

    def per_device(velocity, pressure, force, viscosity, element_stiffness, element_divergence):
        ea, eb, lanes = viscosity.shape
        na, nb = velocity.shape[1], velocity.shape[2]
        dims = (n_patch, n_shell, ea, eb, na, nb, lanes)
        block = 3 * nb
        width = -(-(na + 1) * block // 128) * 128
        g_rows = (nb + 1) * (na + 1) * SLOTS
        vmem = pl.BlockSpec(memory_space=pltpu.VMEM)
        return pl.pallas_call(
            functools.partial(kernel, dims),
            out_shape=(jax.ShapeDtypeStruct(velocity.shape, F32),
                       jax.ShapeDtypeStruct(pressure.shape, F32)),
            in_specs=[pl.BlockSpec(memory_space=pl.ANY)] * 7,
            out_specs=(vmem, vmem),
            scratch_shapes=[
                pltpu.VMEM(velocity.shape, F32),
                pltpu.VMEM(pressure.shape, F32),
                pltpu.VMEM(force.shape, F32),
                pltpu.VMEM(viscosity.shape, F32),
                pltpu.VMEM(element_stiffness.shape, F32),
                pltpu.VMEM(element_divergence.shape, F32),
                pltpu.VMEM(row_map.shape, F32),
                pltpu.SemaphoreType.DMA((7,)),
                pltpu.VMEM((g_rows, lanes), F32),
                pltpu.VMEM((g_rows, lanes), BF16),
                pltpu.VMEM((g_rows, lanes), BF16),
                pltpu.VMEM((g_rows, lanes), F32),
                pltpu.VMEM((g_rows, lanes), F32),
                pltpu.VMEM((ea * eb * 8, lanes), F32),
                pltpu.VMEM((3, ea * eb * 8, lanes), F32),
                pltpu.VMEM((3, nb, 2 * lanes), F32),
                pltpu.VMEM((8, width), F32),
                pltpu.VMEM((8, width), F32),
                pltpu.VMEM((8, width), F32),
                pltpu.VMEM((2, 3, 1, width), F32),
                pltpu.VMEM((3, 3, 3, 1, width), F32),
                pltpu.VMEM((2, 3, 2, block, lanes), F32),
                pltpu.VMEM((2, 3, 2, block, lanes), F32),
                pltpu.VMEM((2, inner * n_shell, 2, lanes), F32),
                pltpu.VMEM((2, n_patch // inner, 2, lanes), F32),
                pltpu.SemaphoreType.DMA((3,)),
                pltpu.SemaphoreType.DMA((3,)),
                pltpu.SemaphoreType.DMA((3, 10)),
                pltpu.SemaphoreType.DMA((3, 10)),
                pltpu.SemaphoreType.DMA((2, 2)),
                pltpu.SemaphoreType.DMA((2, 2)),
            ],
            compiler_params=pltpu.CompilerParams(collective_id=0, has_side_effects=True),
        )(velocity, pressure, force, viscosity, element_stiffness, element_divergence,
          jnp.asarray(row_map))

    spec = P(None, "patch", None, "shell")
    return jax.shard_map(
        per_device,
        mesh=mesh,
        in_specs=(spec, spec, spec, P("patch", None, "shell"), P(), P()),
        out_specs=(spec, spec),
        check_vma=False,
    )
```
